32 devices in a mesh: groups: 2 (over y), branch: 4 (over z), leaf: 4 (over x, core).
Axes of the slice: x: 2, y: 2, z: 4, core: 2. Of those that a mesh axis runs over, the one named last changes fastest.
Arguments:
- queries: float32 [4096, 1024], P(('groups', 'branch', 'leaf')), parts along dimension 0, may hold values from -32 to 32
- leaf_keys: float32 [4096, 128], P(('groups', 'branch', 'leaf')), parts along dimension 0, may hold values from -6 to 6
- leaf_values: float32 [4096, 128], P(('groups', 'branch', 'leaf')), parts along dimension 0, may hold values from -6 to 6
- root_keys: float32 [512, 128], P(('groups', 'branch', 'leaf')), parts along dimension 0, may hold values from -12 to 12
- root_values: float32 [512, 128], P(('groups', 'branch', 'leaf')), parts along dimension 0, may hold values from -6 to 6
- branch_keys: float32 [2048, 128], P(('groups', 'branch', 'leaf')), parts along dimension 0, may hold values from -6 to 6
- branch_values: float32 [2048, 128], P(('groups', 'branch', 'leaf')), parts along dimension 0, may hold values from -6 to 6
- d_out: float32 [4096, 1024], P(('groups', 'branch', 'leaf')), parts along dimension 0, may hold values from -6 to 6
- leaf_len: int32 [32], P(('groups', 'branch', 'leaf')), parts along dimension 0, may hold values from 1 to 128, 1280 in all
- leaf_parent: int32 [32], P(('groups', 'branch', 'leaf')), parts along dimension 0, may hold values from 0 to 255
- root_cut: int32 [8], P(('groups', 'branch')), parts along dimension 0, may hold values from 128 to 256
Outputs:
- attended: float32 [4096, 1024], P(('groups', 'branch', 'leaf')), parts along dimension 0
- d_queries: float32 [4096, 1024], P(('groups', 'branch', 'leaf')), parts along dimension 0
- d_root_kv: float32 [512, 256], P(('groups', 'branch', 'leaf')), parts along dimension 0
- d_branch_kv: float32 [2048, 256], P(('groups', 'branch', 'leaf')), parts along dimension 0
- d_leaf_kv: float32 [4096, 256], P(('groups', 'branch', 'leaf')), parts along dimension 0
The draws below stay inside these ranges and needn't reach their ends.
There are 2 independent parts, one for each index of `groups`. The reference program is written for one: setup_inputs(seed, part) draws one part's arguments, and reference() takes and returns one part's arrays. A program takes and returns all parts, laid end to end along the dimension named above; each array names one. Nothing has to cross between parts.
Inputs may be any that keep to these rules, and one draw needn't show every extreme that they name: `leaf_len`: the lengths of one tree sum to 1280, and some leaf holds 128 live tokens.
All inputs are finite; a program needn't handle non-finite values. No bound on the sum of `leaf_len` on one device may be relied on, other than what follows from the above.
Results may differ from the reference program's by a relative error of at most 0.0003.
Values sent between devices are 32-bit elements; how exact they have to be, the bound alone decides.
A program may use at most 64 MiB of HBM per device.

```python
import math
import jax
import jax.numpy as jnp
import numpy as np
from jax import lax

HEAD_DIM = 128
HEADS = 8
LEAF_CAP = 128
ROOT = 256
BRANCH = 256
BRANCH_ALL = 1024
LEAVES = 16
LEAF_TOTAL = 2048
N_BRANCH = 4
N_LEAF = 4


def draw_root_keys(key, part):
    noise_key = jax.random.fold_in(jax.random.fold_in(key, 11), 0)
    entries = jnp.clip(jax.random.normal(noise_key, (ROOT, HEAD_DIM), jnp.float32), -4.0, 4.0)
    return entries.astype(jnp.float32)


def draw_queries(key, part):
    noise_key = jax.random.fold_in(jax.random.fold_in(key, 23), 0)
    entries = 2.5 * jnp.clip(jax.random.normal(noise_key, (LEAF_TOTAL, HEADS, HEAD_DIM), jnp.float32), -4.0, 4.0)
    return entries.reshape(LEAF_TOTAL, HEADS * HEAD_DIM).astype(jnp.float32)


def touch_ends(drawn, own_key, low, top_value):
    longest = drawn.shape.index(max(drawn.shape))
    spots = []
    for shift in (0, 1):
        where = [jax.random.randint(jax.random.fold_in(own_key, axis), (), 0, length) for axis, length in enumerate(drawn.shape)]
        where[longest] = (where[longest] + shift) % drawn.shape[longest]
        spots.append(tuple(where))
    return drawn.at[spots[0]].set(low).at[spots[1]].set(top_value)


def level_of(stream_key, dims, cuts, low, high):
    level = 1.0
    for position, parts in cuts:
        heights = jax.random.uniform(jax.random.fold_in(jax.random.fold_in(stream_key, 6), position), (parts,), jnp.float32, low / len(cuts), high / len(cuts))
        level = level * jnp.repeat(jnp.exp(heights), dims[position] // parts).reshape((-1,) + (1,) * (len(dims) - 1 - position))
    return level


def profile(number_of, total, reach, skew):
    weights = [(1 << 20) // math.isqrt(standing ** skew) + 1 for standing in range(2, number_of + 1)]
    surplus, counts = total - reach - (number_of - 1), [1] * (number_of - 1)
    while surplus > 0:
        free = [i for i in range(number_of - 1) if counts[i] < reach]
        whole, left = sum([weights[i] for i in free]), surplus
        for i in free:
            more = min(reach - counts[i], max(1, left * weights[i] // whole), surplus)
            counts[i] = counts[i] + more
            surplus = surplus - more
    return np.array([reach] + counts)


def uneven_parts(own_key, number_of, total, limit, lean):
    if number_of == 2:
        one = jax.random.randint(own_key, (), max(1, total - limit), min(limit, total - 1) + 1)
        return jnp.stack([one, total - one])
    sizes = jnp.asarray(profile(number_of, total, limit, lean), jnp.int32)
    pairs = (number_of - 1) // 2
    giver, sink = sizes[1:1 + 2 * pairs:2], sizes[2:2 + 2 * pairs:2]
    margin = jnp.minimum(giver - 1, limit - sink)
    shifted = jax.random.randint(jax.random.fold_in(own_key, 1), (pairs,), 0, 1 << 20) % (margin + 1)
    sizes = sizes.at[1:1 + 2 * pairs:2].set(giver - shifted).at[2:2 + 2 * pairs:2].set(sink + shifted)
    return sizes[jax.random.permutation(jax.random.fold_in(own_key, 2), number_of)]


def normal_values(key, extent, scale, limit, cuts=(), kind=jnp.bfloat16):
    gain = level_of(key, extent, cuts, -0.22, 0.18) if cuts else 1.0
    values = jax.random.normal(key, extent, jnp.float32) * scale * gain
    return jnp.minimum(jnp.maximum(values, -limit), limit).astype(kind)


def setup_inputs(seed: int = 0, part: int = 0) -> dict:
    key_list = jax.random.split(jax.random.key(seed), 12)
    part_splits = jax.random.split(jax.random.fold_in(key_list[11], part), 12)
    return {
        "queries": draw_queries(jax.random.fold_in(jax.random.fold_in(key_list[11], part), 71), part),
        "leaf_keys": normal_values(part_splits[1], (LEAF_TOTAL, HEAD_DIM), 1.5, 6.0, ((0, 16),), jnp.float32),
        "leaf_values": normal_values(part_splits[2], (LEAF_TOTAL, HEAD_DIM), 1.0, 6.0, ((0, 16),), jnp.float32),
        "root_keys": draw_root_keys(jax.random.fold_in(jax.random.fold_in(key_list[11], part), 71), part),
        "root_values": normal_values(part_splits[4], (ROOT, HEAD_DIM), 1.0, 6.0, ((0, 16),), jnp.float32),
        "branch_keys": normal_values(part_splits[5], (BRANCH_ALL, HEAD_DIM), 1.0, 6.0, ((0, 16),), jnp.float32),
        "branch_values": normal_values(part_splits[6], (BRANCH_ALL, HEAD_DIM), 1.0, 6.0, ((0, 16),), jnp.float32),
        "d_out": normal_values(part_splits[7], (LEAF_TOTAL, HEADS * HEAD_DIM), 1.0, 6.0, ((0, 16),), jnp.float32),
        "leaf_len": uneven_parts(part_splits[8], LEAVES, LEAVES * (5 * LEAF_CAP // 8), LEAF_CAP, 2).astype(jnp.int32),
        "leaf_parent": touch_ends(jax.random.randint(part_splits[9], (LEAVES,), 0, BRANCH), jax.random.fold_in(part_splits[9], 1), 0, BRANCH - 1).astype(jnp.int32),
        "root_cut": touch_ends(jax.random.randint(part_splits[10], (N_BRANCH,), ROOT // 2, ROOT + 1), jax.random.fold_in(part_splits[10], 1), ROOT // 2, ROOT).astype(jnp.int32),
    }


def leaf_attention(query_heads, whole_root_keys, whole_root_values, slice_keys, slice_values, own_keys, own_values, root_limit, parent, length):
    head_dim = own_keys.shape[1]
    score_scale = 1.0 / math.sqrt(head_dim)
    highest = lax.Precision.HIGHEST
    all_keys = jnp.concatenate([whole_root_keys, slice_keys, own_keys], axis=0)
    all_values = jnp.concatenate([whole_root_values, slice_values, own_values], axis=0)
    columns = jnp.arange(all_keys.shape[0], dtype=jnp.int32)[None, :]
    positions = jnp.arange(own_keys.shape[0], dtype=jnp.int32)[:, None]
    in_root = columns < root_limit
    in_slice = (columns >= ROOT) & (columns < ROOT + BRANCH) & (columns - ROOT <= parent)
    in_leaf = (columns >= ROOT + BRANCH) & (columns - ROOT - BRANCH <= positions)
    visible = in_root | in_slice | in_leaf
    scores = jnp.einsum('thd,kd->thk', query_heads, all_keys, precision=highest) * score_scale
    scores = jnp.where(visible[:, None, :], scores, -jnp.inf)
    row_max = lax.stop_gradient(lax.optimization_barrier(jnp.max(scores, axis=-1, keepdims=True)))
    raised = jnp.exp(scores - row_max)
    weights = raised / lax.optimization_barrier(jnp.sum(raised, axis=-1, keepdims=True))
    mixture = jnp.einsum('thk,kd->thd', weights, all_values, precision=highest)
    live_rows = (positions[:, 0] < length).astype(jnp.float32)
    return mixture * live_rows[:, None, None]

def reference(queries, leaf_keys, leaf_values, root_keys, root_values, branch_keys, branch_values, d_out, leaf_len, leaf_parent, root_cut):
    query_all = queries.reshape(LEAVES, LEAF_CAP, HEADS, HEAD_DIM)
    cotangent_all = d_out.reshape(LEAVES, LEAF_CAP, HEADS, HEAD_DIM)
    own_keys_all = leaf_keys.reshape(LEAVES, LEAF_CAP, HEAD_DIM)
    own_values_all = leaf_values.reshape(LEAVES, LEAF_CAP, HEAD_DIM)

    def per_leaf(running, inputs):
        root_total, slice_total = running
        leaf_index, query_heads, own_keys, own_values, cotangent, length, parent = inputs
        slice_index = (leaf_index // N_LEAF).astype(jnp.int32)
        offset = (slice_index * BRANCH).astype(jnp.int32)
        slice_keys = lax.dynamic_slice_in_dim(branch_keys, offset, BRANCH, 0)
        slice_values = lax.dynamic_slice_in_dim(branch_values, offset, BRANCH, 0)
        root_limit = lax.dynamic_index_in_dim(root_cut, slice_index, keepdims=False)

        def forward(query_in, rootk_in, rootv_in, slicek_in, slicev_in, ownk_in, ownv_in):
            return leaf_attention(query_in, rootk_in, rootv_in, slicek_in, slicev_in, ownk_in, ownv_in, root_limit, parent, length)
        mixture, pullback = jax.vjp(forward, query_heads, root_keys, root_values, slice_keys, slice_values, own_keys, own_values)
        gradients = pullback(cotangent)
        root_total = root_total + jnp.concatenate([gradients[1], gradients[2]], axis=1)
        slice_piece = jnp.concatenate([gradients[3], gradients[4]], axis=1)
        current = lax.dynamic_slice_in_dim(slice_total, offset, BRANCH, 0)
        slice_total = lax.dynamic_update_slice_in_dim(slice_total, current + slice_piece, offset, 0)
        outputs = (mixture.reshape(LEAF_CAP, HEADS * HEAD_DIM), gradients[0].reshape(LEAF_CAP, HEADS * HEAD_DIM), jnp.concatenate([gradients[5], gradients[6]], axis=1))
        return ((root_total, slice_total), outputs)
    initial = (jnp.zeros((ROOT, 2 * HEAD_DIM), jnp.float32), jnp.zeros((BRANCH_ALL, 2 * HEAD_DIM), jnp.float32))
    leaf_ids = jnp.arange(LEAVES, dtype=jnp.int32)
    finals, stacked = lax.scan(per_leaf, initial, (leaf_ids, query_all, own_keys_all, own_values_all, cotangent_all, leaf_len, leaf_parent))
    root_total, slice_total = finals
    attended, d_queries, d_leaf = stacked
    return (attended.reshape(LEAF_TOTAL, HEADS * HEAD_DIM), d_queries.reshape(LEAF_TOTAL, HEADS * HEAD_DIM), root_total, slice_total, d_leaf.reshape(LEAF_TOTAL, 2 * HEAD_DIM))
```

```python
import functools
import math

import jax
import jax.numpy as jnp
from jax import lax
from jax.experimental import pallas as pl
from jax.experimental.pallas import tpu as pltpu
from jax.sharding import PartitionSpec as P

f32 = jnp.float32
bf16 = jnp.bfloat16
hidden = -1e30


def split2(x):
    high = x.astype(bf16)
    return high, (x - high.astype(f32)).astype(bf16)


def split3(x):
    high = x.astype(bf16)
    rest = x - high.astype(f32)
    middle = rest.astype(bf16)
    return high, middle, (rest - middle.astype(f32)).astype(bf16)


def mm(a, b):
    return lax.dot_general(a, b, (((1,), (0,)), ((), ())), preferred_element_type=f32)


def mmt(a, b):
    return lax.dot_general(a, b, (((1,), (1,)), ((), ())), preferred_element_type=f32)


def side(*parts):
    return jnp.concatenate(parts, axis=1)


def kernel(
    nb, nx, nc, dims,
    q_hbm, lk_hbm, lv_hbm, rk_hbm, rv_hbm, bk_hbm, bv_hbm, do_hbm, len_hbm, par_hbm, cut_hbm,
    att_ref, dqv_ref, droot_ref, dslice_ref, dleaf_ref,
    qd_ref, leaf_ref, rootb, sliceb,
    qs, cs, qt, ct, ks, vs, kt, vt, sc, dp, dkv, top_c, sum_c, dot_c, fac_c, dot_r,
    len_ref, par_ref, cut_ref,
    rc_root, rc_slice, sn_root, sn_slice, rv_root, rv_slice,
    ld_sem, gs_root, gr_root, gs_slice, gr_slice, cs_sem, cr_sem,
    ss_root, sr_root, ss_slice, sr_slice, es_sem, er_sem,
):
    T, H, D, r_rows, b_rows = dims
    R = T * H
    n_root = nb * nx * nc * r_rows
    n_part = nc * b_rows
    n_slice = nx * n_part
    n_keys = n_root + n_slice + T
    scale = 1.0 / math.sqrt(D)
    g = lax.axis_index("groups")
    b = lax.axis_index("branch")
    leaf = lax.axis_index("leaf")
    x = leaf // nc
    c = leaf % nc
    pair = 2 * T if H % 2 == 0 else T
    per = pair // T
    n_pair = R // pair

    def dev(bb, xx, cc):
        return (g, bb, xx * nc + cc)

    def shifted(sb, sx):
        return lax.rem(b + sb, nb), lax.rem(x + sx, nx)

    peers = [(sb, sx) for sb in range(nb) for sx in range(nx) if sb or sx]
    other = lax.rem(c + 1, nc)

    loads = [
        [(rk_hbm, rootb.at[b, x, c, 0]), (rv_hbm, rootb.at[b, x, c, 1])],
        [(bk_hbm, sliceb.at[x, c, 0]), (bv_hbm, sliceb.at[x, c, 1])],
        [(q_hbm, qd_ref.at[0]), (do_hbm, qd_ref.at[1])],
        [(lk_hbm, leaf_ref.at[0]), (lv_hbm, leaf_ref.at[1])],
        [(len_hbm, len_ref)],
        [(par_hbm, par_ref)],
        [(cut_hbm, cut_ref)],
    ]
    for i, group in enumerate(loads):
        for source, target in group:
            pltpu.make_async_copy(source, target, ld_sem.at[i]).start()

    def loaded(i, target):
        pltpu.make_async_copy(target, target, ld_sem.at[i]).wait()

    barrier = pltpu.get_barrier_semaphore()
    for sb, sx in peers:
        bb, xx = shifted(sb, sx)
        pl.semaphore_signal(barrier, inc=1, device_id=dev(bb, xx, c), device_id_type=pl.DeviceIdType.MESH)
    if nc == 2:
        pl.semaphore_signal(barrier, inc=1, device_id=dev(b, x, other), device_id_type=pl.DeviceIdType.MESH)
    loaded(0, rootb.at[b, x, c])
    loaded(1, sliceb.at[x, c])
    pl.semaphore_wait(barrier, len(peers) + (nc == 2))

    def remote(src, dst, s_sem, r_sem, where):
        return pltpu.make_async_remote_copy(
            src_ref=src, dst_ref=dst, send_sem=s_sem, recv_sem=r_sem,
            device_id=where, device_id_type=pl.DeviceIdType.MESH,
        )

    own = rootb.at[b, x, c]
    for sb, sx in peers:
        bb, xx = shifted(sb, sx)
        remote(own, own, gs_root, gr_root, dev(bb, xx, c)).start()
    own = sliceb.at[x, c]
    for sx in range(1, nx):
        bb, xx = shifted(0, sx)
        remote(own, own, gs_slice, gr_slice.at[sx], dev(b, xx, c)).start()
    core_sends = []

    def to_sibling(ref, i):
        core_sends.append(remote(ref, ref, cs_sem.at[i], cr_sem.at[i], dev(b, x, other)))
        core_sends[-1].start()

    def from_sibling(ref, i):
        remote(ref, ref, cs_sem.at[i], cr_sem.at[i], dev(b, x, other)).wait_recv()

    if nc == 2:
        to_sibling(own, 0)

    loaded(2, qd_ref)
    loaded(3, leaf_ref)
    loaded(4, len_ref)
    loaded(5, par_ref)
    loaded(6, cut_ref)
    live = lax.broadcasted_iota(jnp.int32, (T, D), 0) < len_ref[0]
    for h in range(H):
        cols = slice(h * D, (h + 1) * D)
        rows = slice(h * T, (h + 1) * T)
        q = qd_ref[0, :, cols]
        q1, q2 = split2(q)
        qs[rows, :] = side(q1, q2)
        q1, q2, q3 = split3(q.T)
        qt[0, :D, rows], qt[0, D:, rows] = q1, q1
        qt[1, :D, rows], qt[1, D:, rows] = q2, q2
        qt[2, :D, rows], qt[2, D:, rows] = q3, q1
        d = jnp.where(live, qd_ref[1, :, cols], 0.0)
        c1, c2 = split2(d)
        cs[rows, :] = side(c1, c2)
        c1, c2 = split2(d.T)
        ct[0, :D, rows], ct[0, D:, rows] = c1, c1
        ct[1, :D, rows], ct[1, D:, rows] = c2, c2

    def stage(first, keys, values):
        span = slice(first, first + keys.shape[0])
        k1, k2, k3 = split3(keys)
        ks[span, :] = side(k1, k2, k1, k3)
        v1, v2 = split2(values)
        vs[span, :] = side(v1, v2)

    def stage_across(first, keys, values):
        span = slice(first, first + keys.shape[0])
        ka, kb = split2(keys.T)
        kt[:D, span] = ka
        kt[D:, span] = kb
        va, vb = split2(values.T)
        vt[:D, span] = va
        vt[D:, span] = vb

    def score(chunk, first, count, seen, wide):
        span = slice(first, first + count)
        k12, k13, v12 = ks.at[span, : 2 * D], ks.at[span, 2 * D :], vs.at[span, :]

        def body(p):
            rows = pl.ds(pl.multiple_of(p * pair, pair), pair)
            s = mm(k12[...], qt[0, :, rows]) + (mm(k12[...], qt[1, :, rows]) + mm(k13[...], qt[2, :, rows]))
            s = jnp.where(seen(count), s * scale, hidden)
            m = jnp.max(s, axis=0, keepdims=True)
            g = mm(v12[...], ct[0, :, rows]) + mm(v12[...], ct[1, :, rows])
            e = jnp.exp(s - m)
            sc[span, rows] = e
            dp[span, rows] = g
            top_c[chunk : chunk + 1, rows] = m
            sum_c[chunk : chunk + 1, rows] = jnp.sum(e, axis=0, keepdims=True)
            dot_c[chunk : chunk + 1, rows] = jnp.sum(e * g, axis=0, keepdims=True)

        def trip(i, carry):
            for k in range(wide):
                body(i * wide + k)
            return carry

        if n_pair == wide:
            trip(0, 0)
        else:
            lax.fori_loop(0, n_pair // wide, trip, 0)

    def index_of(step):
        return lax.broadcasted_iota(jnp.int32, (step, pair), 0)

    def slot_of(step):
        return lax.broadcasted_iota(jnp.int32, (step, pair), 1) % T

    step = 256 if n_root % 256 == 0 else 128
    at_leaf = n_root + n_slice
    chunks = [(at_leaf, T)]
    chunks += [(n_root + sx * n_part, n_part) for sx in range(nx)]
    chunks += [(lo, step) for lo in range(0, n_root, step)]
    two = 2 if n_pair % 2 == 0 else 1

    stage(at_leaf, leaf_ref[0], leaf_ref[1])
    score(0, at_leaf, T, lambda step: index_of(step) <= slot_of(step), two)

    def score_part(sx):
        bb, xx = shifted(0, sx)
        first, count = chunks[1 + sx]
        stage(first, sliceb[xx, :, 0].reshape(count, D), sliceb[xx, :, 1].reshape(count, D))
        score(1 + sx, first, count, lambda step: xx * n_part + index_of(step) <= par_ref[0], two)

    if nc == 2:
        from_sibling(sliceb.at[x, other], 0)
    score_part(0)

    for sx in range(1, nx):
        bb, xx = shifted(0, nx - sx)
        blk = sliceb.at[xx, c]
        remote(blk, blk, gs_slice, gr_slice.at[sx], dev(b, x, c)).wait_recv()
        if nc == 2:
            to_sibling(blk, 1 + nx - sx)
    remote(rv_root, rv_root, gs_root, gr_root, dev(b, x, c)).wait_recv()
    if nc == 2:
        to_sibling(rootb.at[:, :, c], 1)
    for sx in range(1, nx):
        bb, xx = shifted(0, sx)
        if nc == 2:
            from_sibling(sliceb.at[xx, other], 1 + sx)
        score_part(sx)
    if nc == 2:
        from_sibling(rootb.at[:, :, other], 1)
    stage(0, rootb[:, :, :, 0].reshape(n_root, D), rootb[:, :, :, 1].reshape(n_root, D))
    for i, (first, count) in enumerate(chunks[1 + nx :]):
        score(
            1 + nx + i, first, count, lambda step: first + index_of(step) < cut_ref[0],
            n_pair if n_root == step else two,
        )

    tops = top_c[...]
    factor = jnp.exp(tops - jnp.max(tops, axis=0, keepdims=True))
    inverse = 1.0 / jnp.sum(factor * sum_c[...], axis=0, keepdims=True)
    fac_c[...] = factor * inverse
    dot_r[...] = jnp.sum(factor * dot_c[...], axis=0, keepdims=True) * inverse

    def weights(chunk, rows):
        first, count = chunks[chunk]
        span = slice(first, first + count)
        w = sc[span, rows] * fac_c[chunk : chunk + 1, rows]
        return split2(w), split2(w * ((dp[span, rows] - dot_r[:, rows]) * scale))

    def key_gradients(chunk):
        (w1, w2), (s1, s2) = weights(chunk, slice(None))
        a = mm(s1, qs[...]) + mm(s2, qs[...])
        v = mm(w1, cs[...]) + mm(w2, cs[...])
        return side(a[:, :D] + a[:, D:], v[:, :D] + v[:, D:])

    def block_gradients(chunk):
        first, count = chunks[chunk]
        dkv[first : first + count, :] = key_gradients(chunk)

    root_g = dkv.at[:n_root].reshape(nb, nx, nc, r_rows, 2 * D)
    slice_g = dkv.at[n_root : n_root + n_slice].reshape(nx, nc, b_rows, 2 * D)
    for i in range(1 + nx, len(chunks)):
        block_gradients(i)
    ex = []
    if nc == 2:
        ex.append(remote(root_g.at[:, :, other], rc_root, es_sem.at[0], er_sem.at[0], dev(b, x, other)))
        ex[0].start()
    for sx in range(nx):
        block_gradients(1 + sx)
    if nc == 2:
        ex.append(remote(slice_g.at[:, other], rc_slice, es_sem.at[1], er_sem.at[1], dev(b, x, other)))
        ex[1].start()
        ex[0].wait_recv()
    mine = root_g[:, :, c]
    sn_root[...] = mine + rc_root[...] if nc == 2 else mine
    for i, (sb, sx) in enumerate(peers):
        bb, xx = shifted(sb, sx)
        remote(sn_root.at[bb, xx], rv_root.at[i], ss_root, sr_root, dev(bb, xx, c)).start()

    stage_across(0, rootb[:, :, :, 0].reshape(n_root, D), rootb[:, :, :, 1].reshape(n_root, D))
    for sx in range(nx):
        bb, xx = shifted(0, sx)
        first, count = chunks[1 + sx]
        stage_across(first, sliceb[xx, :, 0].reshape(count, D), sliceb[xx, :, 1].reshape(count, D))
    stage_across(at_leaf, leaf_ref[0], leaf_ref[1])

    if nc == 2:
        ex[1].wait_recv()
    mine = slice_g[:, c]
    sn_slice[...] = mine + rc_slice[...] if nc == 2 else mine
    for sx in range(1, nx):
        bb, xx = shifted(0, sx)
        remote(sn_slice.at[sx], rv_slice.at[sx - 1], ss_slice, sr_slice, dev(b, xx, c)).start()

    def outputs(p, carry):
        rows = pl.ds(pl.multiple_of(p * pair, pair), pair)
        m, n = None, None
        for chunk, (first, count) in enumerate(chunks):
            span = slice(first, first + count)
            (w1, w2), (s1, s2) = weights(chunk, rows)
            part = mm(vt[:, span], w1) + mm(vt[:, span], w2)
            m = part if m is None else m + part
            part = mm(kt[:, span], s1) + mm(kt[:, span], s2)
            n = part if n is None else n + part
        m = m[:D] + m[D:]
        n = n[:D] + n[D:]
        for k in range(per):
            cols = pl.ds(pl.multiple_of(p * (per * D) + k * D, D), D)
            part = slice(k * T, (k + 1) * T)
            att_ref[:, cols] = jnp.where(live, m[:, part].T, 0.0)
            dqv_ref[:, cols] = n[:, part].T
        return carry

    lax.fori_loop(0, n_pair, outputs, 0)
    dleaf_ref[...] = key_gradients(0)

    total = sn_slice[0]
    if nx > 1:
        remote(rv_slice, rv_slice, ss_slice, sr_slice, dev(b, x, c)).wait_recv()
        for i in range(nx - 1):
            total = total + rv_slice[i]
    dslice_ref[...] = total
    total = sn_root[b, x]
    if peers:
        remote(rv_root, rv_root, ss_root, sr_root, dev(b, x, c)).wait_recv()
        for i in range(len(peers)):
            total = total + rv_root[i]
    droot_ref[...] = total
    for cp in core_sends + ex:
        cp.wait_send()
    if peers:
        remote(rv_root, rv_root, gs_root, gr_root, dev(b, x, c)).wait_send()
        remote(rv_root, rv_root, ss_root, sr_root, dev(b, x, c)).wait_send()
    if nx > 1:
        remote(rv_slice, rv_slice, gs_slice, gr_slice.at[0], dev(b, x, c)).wait_send()
        remote(rv_slice, rv_slice, ss_slice, sr_slice, dev(b, x, c)).wait_send()


def deliver(*refs):
    sources, targets, sem = refs[:5], refs[5:10], refs[10]
    copies = [pltpu.make_async_copy(s, t, sem.at[i]) for i, (s, t) in enumerate(zip(sources, targets))]
    for cp in copies:
        cp.start()
    for cp in copies:
        cp.wait()


def shards(mesh, *args):
    queries, leaf_keys, _, root_keys, _, branch_keys = args[:6]
    T, width = queries.shape
    D = leaf_keys.shape[1]
    H = width // D
    r_rows, b_rows = root_keys.shape[0], branch_keys.shape[0]
    nb, nl = mesh.shape["branch"], mesh.shape["leaf"]
    nc = 2 if nl % 2 == 0 else 1
    nx = nl // nc
    R = T * H
    n_root, n_slice = nb * nl * r_rows, nl * b_rows
    n_keys = n_root + n_slice + T
    n_chunks = 1 + nx + n_root // (256 if n_root % 256 == 0 else 128)
    any_space = pl.BlockSpec(memory_space=pl.ANY)
    hbm = pl.BlockSpec(memory_space=pltpu.HBM)
    vmem = pl.BlockSpec(memory_space=pltpu.VMEM)
    V = pltpu.VMEM
    S = pltpu.SMEM
    dma = pltpu.SemaphoreType.DMA
    np_ = max(nb * nx - 1, 1)
    scratch = [
        V((2, T, width), f32), V((2, T, D), f32),
        V((nb, nx, nc, 2, r_rows, D), f32), V((nx, nc, 2, b_rows, D), f32),
        V((R, 2 * D), bf16), V((R, 2 * D), bf16), V((3, 2 * D, R), bf16), V((2, 2 * D, R), bf16),
        V((n_keys, 4 * D), bf16), V((n_keys, 2 * D), bf16),
        V((2 * D, n_keys), bf16), V((2 * D, n_keys), bf16),
        V((n_keys, R), f32), V((n_keys, R), f32), V((n_root + n_slice, 2 * D), f32),
        V((n_chunks, R), f32), V((n_chunks, R), f32), V((n_chunks, R), f32), V((n_chunks, R), f32), V((1, R), f32),
        S((1,), jnp.int32), S((1,), jnp.int32), S((1,), jnp.int32),
        V((nb, nx, r_rows, 2 * D), f32), V((nx, b_rows, 2 * D), f32),
        V((nb, nx, r_rows, 2 * D), f32), V((nx, b_rows, 2 * D), f32),
        V((np_, r_rows, 2 * D), f32), V((max(nx - 1, 1), b_rows, 2 * D), f32),
        dma((7,)), dma, dma, dma, dma((nx,)), dma((1 + nx,)), dma((1 + nx,)),
        dma, dma, dma, dma, dma((2,)), dma((2,)),
    ]
    shape = lambda *s: V(s, f32)
    sizes = ((T, width), (T, width), (r_rows, 2 * D), (b_rows, 2 * D), (T, 2 * D))
    held = pl.pallas_call(
        functools.partial(kernel, nb, nx, nc, (T, H, D, r_rows, b_rows)),
        out_shape=tuple(shape(*size) for size in sizes),
        in_specs=[any_space] * 8 + [hbm] * 3,
        out_specs=(vmem,) * 5,
        scratch_shapes=scratch,
        compiler_params=pltpu.CompilerParams(
            collective_id=0, has_side_effects=True, vmem_limit_bytes=60 * 1024 * 1024
        ),
        name="tree",
    )(*args)
    return pl.pallas_call(
        deliver,
        out_shape=tuple(jax.ShapeDtypeStruct(size, f32) for size in sizes),
        in_specs=[vmem] * 5,
        out_specs=(any_space,) * 5,
        scratch_shapes=[dma((5,))],
        compiler_params=pltpu.CompilerParams(vmem_limit_bytes=1024 * 1024),
        name="deliver",
    )(*held)


def solution(mesh):
    rows = P(("groups", "branch", "leaf"), None)
    flat = P(("groups", "branch", "leaf"))
    return jax.shard_map(
        functools.partial(shards, mesh),
        mesh=mesh,
        in_specs=(rows,) * 8 + (flat, flat, P(("groups", "branch"))),
        out_specs=(rows,) * 5,
        check_vma=False,
    )
```

```python
import functools
import math

import jax
import jax.numpy as jnp
from jax import lax
from jax.experimental import pallas as pl
from jax.experimental.pallas import tpu as pltpu
from jax.sharding import PartitionSpec as P

f32 = jnp.float32
bf16 = jnp.bfloat16
hidden = -1e30


def split2(x):
    high = x.astype(bf16)
    return high, (x - high.astype(f32)).astype(bf16)


def split3(x):
    high = x.astype(bf16)
    rest = x - high.astype(f32)
    middle = rest.astype(bf16)
    return high, middle, (rest - middle.astype(f32)).astype(bf16)


def mm(a, b):
    return lax.dot_general(a, b, (((1,), (0,)), ((), ())), preferred_element_type=f32)


def mmt(a, b):
    return lax.dot_general(a, b, (((1,), (1,)), ((), ())), preferred_element_type=f32)


def side(*parts):
    return jnp.concatenate(parts, axis=1)


def kernel(
    nb, nx, nc, dims,
    q_hbm, lk_hbm, lv_hbm, rk_hbm, rv_hbm, bk_hbm, bv_hbm, do_hbm, len_hbm, par_hbm, cut_hbm,
    att_ref, dqv_ref, droot_ref, dslice_ref, dleaf_ref,
    qd_ref, leaf_ref, rootb, sliceb,
    qs, cs, qt, ct, ks, vs, kt, vt, sc, dp, dkv, top_c, sum_c, dot_c, fac_c, dot_r,
    len_ref, par_ref, cut_ref,
    rc_root, rc_slice, sn_root, sn_slice, rv_root, rv_slice,
    ld_sem, gs_root, gr_root, gs_slice, gr_slice, cs_sem, cr_sem,
    ss_root, sr_root, ss_slice, sr_slice, es_sem, er_sem,
):
    T, H, D, r_rows, b_rows = dims
    R = T * H
    n_root = nb * nx * nc * r_rows
    n_part = nc * b_rows
    n_slice = nx * n_part
    n_keys = n_root + n_slice + T
    scale = 1.0 / math.sqrt(D)
    g = lax.axis_index("groups")
    b = lax.axis_index("branch")
    leaf = lax.axis_index("leaf")
    x = leaf // nc
    c = leaf % nc
    pair = 2 * T if H % 2 == 0 else T
    per = pair // T
    n_pair = R // pair

    def dev(bb, xx, cc):
        return (g, bb, xx * nc + cc)

    def shifted(sb, sx):
        return lax.rem(b + sb, nb), lax.rem(x + sx, nx)

    peers = [(sb, sx) for sb in range(nb) for sx in range(nx) if sb or sx]
    peers.sort(key=lambda p: (p[1] == 0, -min(p[0], nb - p[0])))
    other = lax.rem(c + 1, nc)

    loads = [
        [(rk_hbm, rootb.at[b, x, c, 0]), (rv_hbm, rootb.at[b, x, c, 1])],
        [(bk_hbm, sliceb.at[x, c, 0]), (bv_hbm, sliceb.at[x, c, 1])],
        [(q_hbm, qd_ref.at[0]), (do_hbm, qd_ref.at[1])],
        [(lk_hbm, leaf_ref.at[0]), (lv_hbm, leaf_ref.at[1])],
        [(len_hbm, len_ref)],
        [(par_hbm, par_ref)],
        [(cut_hbm, cut_ref)],
    ]
    for i, group in enumerate(loads):
        for source, target in group:
            pltpu.make_async_copy(source, target, ld_sem.at[i]).start()

    def loaded(i, target):
        pltpu.make_async_copy(target, target, ld_sem.at[i]).wait()

    barrier = pltpu.get_barrier_semaphore()
    for sb, sx in peers:
        bb, xx = shifted(sb, sx)
        pl.semaphore_signal(barrier, inc=1, device_id=dev(bb, xx, c), device_id_type=pl.DeviceIdType.MESH)
    if nc == 2:
        pl.semaphore_signal(barrier, inc=1, device_id=dev(b, x, other), device_id_type=pl.DeviceIdType.MESH)
    loaded(0, rootb.at[b, x, c])
    loaded(1, sliceb.at[x, c])
    pl.semaphore_wait(barrier, len(peers) + (nc == 2))

    def remote(src, dst, s_sem, r_sem, where):
        return pltpu.make_async_remote_copy(
            src_ref=src, dst_ref=dst, send_sem=s_sem, recv_sem=r_sem,
            device_id=where, device_id_type=pl.DeviceIdType.MESH,
        )

    own = rootb.at[b, x, c]
    for sb, sx in peers:
        bb, xx = shifted(sb, sx)
        remote(own, own, gs_root, gr_root, dev(bb, xx, c)).start()
    own = sliceb.at[x, c]
    for sx in range(1, nx):
        bb, xx = shifted(0, sx)
        remote(own, own, gs_slice, gr_slice.at[sx], dev(b, xx, c)).start()
    core_sends = []

    def to_sibling(ref, i):
        core_sends.append(remote(ref, ref, cs_sem.at[i], cr_sem.at[i], dev(b, x, other)))
        core_sends[-1].start()

    def from_sibling(ref, i):
        remote(ref, ref, cs_sem.at[i], cr_sem.at[i], dev(b, x, other)).wait_recv()

    if nc == 2:
        to_sibling(own, 0)

    loaded(2, qd_ref)
    loaded(3, leaf_ref)
    loaded(4, len_ref)
    loaded(5, par_ref)
    loaded(6, cut_ref)
    live = lax.broadcasted_iota(jnp.int32, (T, D), 0) < len_ref[0]
    for h in range(H):
        cols = slice(h * D, (h + 1) * D)
        rows = slice(h * T, (h + 1) * T)
        q = qd_ref[0, :, cols]
        q1, q2 = split2(q)
        qs[rows, :] = side(q1, q2)
        q1, q2, q3 = split3(q.T)
        qt[0, :D, rows], qt[0, D:, rows] = q1, q1
        qt[1, :D, rows], qt[1, D:, rows] = q2, q2
        qt[2, :D, rows], qt[2, D:, rows] = q3, q1
        d = jnp.where(live, qd_ref[1, :, cols], 0.0)
        c1, c2 = split2(d)
        cs[rows, :] = side(c1, c2)
        c1, c2 = split2(d.T)
        ct[0, :D, rows], ct[0, D:, rows] = c1, c1
        ct[1, :D, rows], ct[1, D:, rows] = c2, c2

    def stage(first, keys, values):
        span = slice(first, first + keys.shape[0])
        k1, k2, k3 = split3(keys)
        ks[span, :] = side(k1, k2, k1, k3)
        v1, v2 = split2(values)
        vs[span, :] = side(v1, v2)

    def stage_across(first, keys, values):
        span = slice(first, first + keys.shape[0])
        ka, kb = split2(keys.T)
        kt[:D, span] = ka
        kt[D:, span] = kb
        va, vb = split2(values.T)
        vt[:D, span] = va
        vt[D:, span] = vb

    def score(chunk, first, count, seen, wide):
        span = slice(first, first + count)
        k12, k13, v12 = ks.at[span, : 2 * D], ks.at[span, 2 * D :], vs.at[span, :]

        def body(p):
            rows = pl.ds(pl.multiple_of(p * pair, pair), pair)
            s = mm(k12[...], qt[0, :, rows]) + (mm(k12[...], qt[1, :, rows]) + mm(k13[...], qt[2, :, rows]))
            s = jnp.where(seen(count), s * scale, hidden)
            m = jnp.max(s, axis=0, keepdims=True)
            g = mm(v12[...], ct[0, :, rows]) + mm(v12[...], ct[1, :, rows])
            e = jnp.exp(s - m)
            sc[span, rows] = e
            dp[span, rows] = g
            top_c[chunk : chunk + 1, rows] = m
            sum_c[chunk : chunk + 1, rows] = jnp.sum(e, axis=0, keepdims=True)
            dot_c[chunk : chunk + 1, rows] = jnp.sum(e * g, axis=0, keepdims=True)

        def trip(i, carry):
            for k in range(wide):
                body(i * wide + k)
            return carry

        if n_pair == wide:
            trip(0, 0)
        else:
            lax.fori_loop(0, n_pair // wide, trip, 0)

    def index_of(step):
        return lax.broadcasted_iota(jnp.int32, (step, pair), 0)

    def slot_of(step):
        return lax.broadcasted_iota(jnp.int32, (step, pair), 1) % T

    step = 256 if n_root % 256 == 0 else 128
    at_leaf = n_root + n_slice
    chunks = [(at_leaf, T)]
    chunks += [(n_root + sx * n_part, n_part) for sx in range(nx)]
    chunks += [(lo, step) for lo in range(0, n_root, step)]
    two = 2 if n_pair % 2 == 0 else 1

    stage(at_leaf, leaf_ref[0], leaf_ref[1])
    score(0, at_leaf, T, lambda step: index_of(step) <= slot_of(step), two)

    def score_part(sx):
        bb, xx = shifted(0, sx)
        first, count = chunks[1 + sx]
        stage(first, sliceb[xx, :, 0].reshape(count, D), sliceb[xx, :, 1].reshape(count, D))
        score(1 + sx, first, count, lambda step: xx * n_part + index_of(step) <= par_ref[0], two)

    if nc == 2:
        from_sibling(sliceb.at[x, other], 0)
    score_part(0)

    for sx in range(1, nx):
        bb, xx = shifted(0, nx - sx)
        blk = sliceb.at[xx, c]
        remote(blk, blk, gs_slice, gr_slice.at[sx], dev(b, x, c)).wait_recv()
        if nc == 2:
            to_sibling(blk, 1 + nx - sx)
    remote(rv_root, rv_root, gs_root, gr_root, dev(b, x, c)).wait_recv()
    if nc == 2:
        to_sibling(rootb.at[:, :, c], 1)
    for sx in range(1, nx):
        bb, xx = shifted(0, sx)
        if nc == 2:
            from_sibling(sliceb.at[xx, other], 1 + sx)
        score_part(sx)
    if nc == 2:
        from_sibling(rootb.at[:, :, other], 1)
    stage(0, rootb[:, :, :, 0].reshape(n_root, D), rootb[:, :, :, 1].reshape(n_root, D))
    for i, (first, count) in enumerate(chunks[1 + nx :]):
        score(
            1 + nx + i, first, count, lambda step: first + index_of(step) < cut_ref[0],
            n_pair if n_root == step else two,
        )

    tops = top_c[...]
    factor = jnp.exp(tops - jnp.max(tops, axis=0, keepdims=True))
    inverse = 1.0 / jnp.sum(factor * sum_c[...], axis=0, keepdims=True)
    fac_c[...] = factor * inverse
    dot_r[...] = jnp.sum(factor * dot_c[...], axis=0, keepdims=True) * inverse

    def weights(chunk, rows):
        first, count = chunks[chunk]
        span = slice(first, first + count)
        w = sc[span, rows] * fac_c[chunk : chunk + 1, rows]
        return split2(w), split2(w * ((dp[span, rows] - dot_r[:, rows]) * scale))

    def key_gradients(chunk):
        (w1, w2), (s1, s2) = weights(chunk, slice(None))
        a = mm(s1, qs[...]) + mm(s2, qs[...])
        v = mm(w1, cs[...]) + mm(w2, cs[...])
        return side(a[:, :D] + a[:, D:], v[:, :D] + v[:, D:])

    def block_gradients(chunk):
        first, count = chunks[chunk]
        dkv[first : first + count, :] = key_gradients(chunk)

    root_g = dkv.at[:n_root].reshape(nb, nx, nc, r_rows, 2 * D)
    slice_g = dkv.at[n_root : n_root + n_slice].reshape(nx, nc, b_rows, 2 * D)
    for i in range(1 + nx, len(chunks)):
        block_gradients(i)
    ex = []
    if nc == 2:
        ex.append(remote(root_g.at[:, :, other], rc_root, es_sem.at[0], er_sem.at[0], dev(b, x, other)))
        ex[0].start()
    for sx in range(nx):
        block_gradients(1 + sx)
    if nc == 2:
        ex.append(remote(slice_g.at[:, other], rc_slice, es_sem.at[1], er_sem.at[1], dev(b, x, other)))
        ex[1].start()
        ex[0].wait_recv()
    mine = root_g[:, :, c]
    sn_root[...] = mine + rc_root[...] if nc == 2 else mine
    for i, (sb, sx) in enumerate(peers):
        bb, xx = shifted(sb, sx)
        remote(sn_root.at[bb, xx], rv_root.at[i], ss_root, sr_root, dev(bb, xx, c)).start()

    stage_across(0, rootb[:, :, :, 0].reshape(n_root, D), rootb[:, :, :, 1].reshape(n_root, D))
    for sx in range(nx):
        bb, xx = shifted(0, sx)
        first, count = chunks[1 + sx]
        stage_across(first, sliceb[xx, :, 0].reshape(count, D), sliceb[xx, :, 1].reshape(count, D))
    stage_across(at_leaf, leaf_ref[0], leaf_ref[1])

    if nc == 2:
        ex[1].wait_recv()
    mine = slice_g[:, c]
    sn_slice[...] = mine + rc_slice[...] if nc == 2 else mine
    for sx in range(1, nx):
        bb, xx = shifted(0, sx)
        remote(sn_slice.at[sx], rv_slice.at[sx - 1], ss_slice, sr_slice, dev(b, xx, c)).start()

    def outputs(p, carry):
        rows = pl.ds(pl.multiple_of(p * pair, pair), pair)
        m, n = None, None
        for chunk, (first, count) in enumerate(chunks):
            span = slice(first, first + count)
            (w1, w2), (s1, s2) = weights(chunk, rows)
            part = mm(vt[:, span], w1) + mm(vt[:, span], w2)
            m = part if m is None else m + part
            part = mm(kt[:, span], s1) + mm(kt[:, span], s2)
            n = part if n is None else n + part
        m = m[:D] + m[D:]
        n = n[:D] + n[D:]
        for k in range(per):
            cols = pl.ds(pl.multiple_of(p * (per * D) + k * D, D), D)
            part = slice(k * T, (k + 1) * T)
            att_ref[:, cols] = jnp.where(live, m[:, part].T, 0.0)
            dqv_ref[:, cols] = n[:, part].T
        return carry

    lax.fori_loop(0, n_pair, outputs, 0)
    dleaf_ref[...] = key_gradients(0)

    total = sn_slice[0]
    if nx > 1:
        remote(rv_slice, rv_slice, ss_slice, sr_slice, dev(b, x, c)).wait_recv()
        for i in range(nx - 1):
            total = total + rv_slice[i]
    dslice_ref[...] = total
    total = sn_root[b, x]
    if peers:
        remote(rv_root, rv_root, ss_root, sr_root, dev(b, x, c)).wait_recv()
        for i in range(len(peers)):
            total = total + rv_root[i]
    droot_ref[...] = total
    for cp in core_sends + ex:
        cp.wait_send()
    if peers:
        remote(rv_root, rv_root, gs_root, gr_root, dev(b, x, c)).wait_send()
        remote(rv_root, rv_root, ss_root, sr_root, dev(b, x, c)).wait_send()
    if nx > 1:
        remote(rv_slice, rv_slice, gs_slice, gr_slice.at[0], dev(b, x, c)).wait_send()
        remote(rv_slice, rv_slice, ss_slice, sr_slice, dev(b, x, c)).wait_send()


def deliver(*refs):
    sources, targets, sem = refs[:5], refs[5:10], refs[10]
    copies = [pltpu.make_async_copy(s, t, sem.at[i]) for i, (s, t) in enumerate(zip(sources, targets))]
    for cp in copies:
        cp.start()
    for cp in copies:
        cp.wait()


def shards(mesh, *args):
    queries, leaf_keys, _, root_keys, _, branch_keys = args[:6]
    T, width = queries.shape
    D = leaf_keys.shape[1]
    H = width // D
    r_rows, b_rows = root_keys.shape[0], branch_keys.shape[0]
    nb, nl = mesh.shape["branch"], mesh.shape["leaf"]
    nc = 2 if nl % 2 == 0 else 1
    nx = nl // nc
    R = T * H
    n_root, n_slice = nb * nl * r_rows, nl * b_rows
    n_keys = n_root + n_slice + T
    n_chunks = 1 + nx + n_root // (256 if n_root % 256 == 0 else 128)
    any_space = pl.BlockSpec(memory_space=pl.ANY)
    hbm = pl.BlockSpec(memory_space=pltpu.HBM)
    vmem = pl.BlockSpec(memory_space=pltpu.VMEM)
    V = pltpu.VMEM
    S = pltpu.SMEM
    dma = pltpu.SemaphoreType.DMA
    np_ = max(nb * nx - 1, 1)
    scratch = [
        V((2, T, width), f32), V((2, T, D), f32),
        V((nb, nx, nc, 2, r_rows, D), f32), V((nx, nc, 2, b_rows, D), f32),
        V((R, 2 * D), bf16), V((R, 2 * D), bf16), V((3, 2 * D, R), bf16), V((2, 2 * D, R), bf16),
        V((n_keys, 4 * D), bf16), V((n_keys, 2 * D), bf16),
        V((2 * D, n_keys), bf16), V((2 * D, n_keys), bf16),
        V((n_keys, R), f32), V((n_keys, R), f32), V((n_root + n_slice, 2 * D), f32),
        V((n_chunks, R), f32), V((n_chunks, R), f32), V((n_chunks, R), f32), V((n_chunks, R), f32), V((1, R), f32),
        S((1,), jnp.int32), S((1,), jnp.int32), S((1,), jnp.int32),
        V((nb, nx, r_rows, 2 * D), f32), V((nx, b_rows, 2 * D), f32),
        V((nb, nx, r_rows, 2 * D), f32), V((nx, b_rows, 2 * D), f32),
        V((np_, r_rows, 2 * D), f32), V((max(nx - 1, 1), b_rows, 2 * D), f32),
        dma((7,)), dma, dma, dma, dma((nx,)), dma((1 + nx,)), dma((1 + nx,)),
        dma, dma, dma, dma, dma((2,)), dma((2,)),
    ]
    shape = lambda *s: V(s, f32)
    sizes = ((T, width), (T, width), (r_rows, 2 * D), (b_rows, 2 * D), (T, 2 * D))
    held = pl.pallas_call(
        functools.partial(kernel, nb, nx, nc, (T, H, D, r_rows, b_rows)),
        out_shape=tuple(shape(*size) for size in sizes),
        in_specs=[any_space] * 8 + [hbm] * 3,
        out_specs=(vmem,) * 5,
        scratch_shapes=scratch,
        compiler_params=pltpu.CompilerParams(
            collective_id=0, has_side_effects=True, vmem_limit_bytes=60 * 1024 * 1024
        ),
        name="tree",
    )(*args)
    return pl.pallas_call(
        deliver,
        out_shape=tuple(jax.ShapeDtypeStruct(size, f32) for size in sizes),
        in_specs=[vmem] * 5,
        out_specs=(any_space,) * 5,
        scratch_shapes=[dma((5,))],
        compiler_params=pltpu.CompilerParams(vmem_limit_bytes=1024 * 1024),
        name="deliver",
    )(*held)


def solution(mesh):
    rows = P(("groups", "branch", "leaf"), None)
    flat = P(("groups", "branch", "leaf"))
    return jax.shard_map(
        functools.partial(shards, mesh),
        mesh=mesh,
        in_specs=(rows,) * 8 + (flat, flat, P(("groups", "branch"))),
        out_specs=(rows,) * 5,
        check_vma=False,
    )
```

```python
import functools
import math

import jax
import jax.numpy as jnp
from jax import lax
from jax.experimental import pallas as pl
from jax.experimental.pallas import tpu as pltpu
from jax.sharding import PartitionSpec as P

f32 = jnp.float32
bf16 = jnp.bfloat16
hidden = -1e30


def split2(x):
    high = x.astype(bf16)
    return high, (x - high.astype(f32)).astype(bf16)


def split3(x):
    high = x.astype(bf16)
    rest = x - high.astype(f32)
    middle = rest.astype(bf16)
    return high, middle, (rest - middle.astype(f32)).astype(bf16)


def mm(a, b):
    return lax.dot_general(a, b, (((1,), (0,)), ((), ())), preferred_element_type=f32)


def mmt(a, b):
    return lax.dot_general(a, b, (((1,), (1,)), ((), ())), preferred_element_type=f32)


def side(*parts):
    return jnp.concatenate(parts, axis=1)


def kernel(
    nb, nx, nc, dims,
    q_hbm, lk_hbm, lv_hbm, rk_hbm, rv_hbm, bk_hbm, bv_hbm, do_hbm, len_hbm, par_hbm, cut_hbm,
    att_ref, dqv_ref, droot_ref, dslice_ref, dleaf_ref,
    qd_ref, leaf_ref, rootb, sliceb,
    qs, cs, qt, ct, ks, vs, kt, vt, sc, dp, dkv, top_c, sum_c, dot_c, fac_c, dot_r,
    len_ref, par_ref, cut_ref,
    rc_root, rc_slice, sn_root, sn_slice, rv_root, rv_slice,
    ld_sem, gs_root, gr_root, gs_slice, gr_slice, cs_sem, cr_sem,
    ss_root, sr_root, ss_slice, sr_slice, es_sem, er_sem,
):
    T, H, D, r_rows, b_rows = dims
    R = T * H
    n_root = nb * nx * nc * r_rows
    n_part = nc * b_rows
    n_slice = nx * n_part
    n_keys = n_root + n_slice + T
    scale = 1.0 / math.sqrt(D)
    g = lax.axis_index("groups")
    b = lax.axis_index("branch")
    leaf = lax.axis_index("leaf")
    x = leaf // nc
    c = leaf % nc
    pair = 2 * T if H % 2 == 0 else T
    per = pair // T
    n_pair = R // pair

    def dev(bb, xx, cc):
        return (g, bb, xx * nc + cc)

    def shifted(sb, sx):
        return lax.rem(b + sb, nb), lax.rem(x + sx, nx)

    peers = [(sb, sx) for sb in range(nb) for sx in range(nx) if sb or sx]
    peers.sort(key=lambda p: (p[1] == 0, -min(p[0], nb - p[0])))
    columns = list(range(1, nx)) + [0]
    other = lax.rem(c + 1, nc)

    loads = [
        [(rk_hbm, rootb.at[b, x, c, 0]), (rv_hbm, rootb.at[b, x, c, 1])],
        [(bk_hbm, sliceb.at[x, c, 0]), (bv_hbm, sliceb.at[x, c, 1])],
        [(q_hbm, qd_ref.at[0]), (do_hbm, qd_ref.at[1])],
        [(lk_hbm, leaf_ref.at[0]), (lv_hbm, leaf_ref.at[1])],
        [(len_hbm, len_ref)],
        [(par_hbm, par_ref)],
        [(cut_hbm, cut_ref)],
    ]
    for i, group in enumerate(loads):
        for source, target in group:
            pltpu.make_async_copy(source, target, ld_sem.at[i]).start()

    def loaded(i, target):
        pltpu.make_async_copy(target, target, ld_sem.at[i]).wait()

    barrier = pltpu.get_barrier_semaphore()
    for sb, sx in peers:
        bb, xx = shifted(sb, sx)
        pl.semaphore_signal(barrier, inc=1, device_id=dev(bb, xx, c), device_id_type=pl.DeviceIdType.MESH)
    if nc == 2:
        pl.semaphore_signal(barrier, inc=1, device_id=dev(b, x, other), device_id_type=pl.DeviceIdType.MESH)
    loaded(0, rootb.at[b, x, c])
    pl.semaphore_wait(barrier, len(peers) + (nc == 2))

    def remote(src, dst, s_sem, r_sem, where):
        return pltpu.make_async_remote_copy(
            src_ref=src, dst_ref=dst, send_sem=s_sem, recv_sem=r_sem,
            device_id=where, device_id_type=pl.DeviceIdType.MESH,
        )

    own = rootb.at[b, x, c]
    for sb, sx in peers:
        bb, xx = shifted(sb, sx)
        remote(own, own, gs_root, gr_root, dev(bb, xx, c)).start()
    loaded(1, sliceb.at[x, c])
    own = sliceb.at[x, c]
    for sx in range(1, nx):
        bb, xx = shifted(0, sx)
        remote(own, own, gs_slice, gr_slice.at[sx], dev(b, xx, c)).start()
    core_sends = []

    def to_sibling(ref, i):
        core_sends.append(remote(ref, ref, cs_sem.at[i], cr_sem.at[i], dev(b, x, other)))
        core_sends[-1].start()

    def from_sibling(ref, i):
        remote(ref, ref, cs_sem.at[i], cr_sem.at[i], dev(b, x, other)).wait_recv()

    if nc == 2:
        to_sibling(own, 0)

    loaded(2, qd_ref)
    loaded(3, leaf_ref)
    loaded(4, len_ref)
    loaded(5, par_ref)
    loaded(6, cut_ref)
    live = lax.broadcasted_iota(jnp.int32, (T, D), 0) < len_ref[0]
    for h in range(H):
        cols = slice(h * D, (h + 1) * D)
        rows = slice(h * T, (h + 1) * T)
        q = qd_ref[0, :, cols]
        q1, q2 = split2(q)
        qs[rows, :] = side(q1, q2)
        q1, q2, q3 = split3(q.T)
        qt[0, :D, rows], qt[0, D:, rows] = q1, q1
        qt[1, :D, rows], qt[1, D:, rows] = q2, q2
        qt[2, :D, rows], qt[2, D:, rows] = q3, q1
        d = jnp.where(live, qd_ref[1, :, cols], 0.0)
        c1, c2 = split2(d)
        cs[rows, :] = side(c1, c2)
        c1, c2 = split2(d.T)
        ct[0, :D, rows], ct[0, D:, rows] = c1, c1
        ct[1, :D, rows], ct[1, D:, rows] = c2, c2

    def stage(first, keys, values):
        span = slice(first, first + keys.shape[0])
        k1, k2, k3 = split3(keys)
        ks[span, :] = side(k1, k2, k1, k3)
        v1, v2 = split2(values)
        vs[span, :] = side(v1, v2)

    def stage_across(first, keys, values):
        span = slice(first, first + keys.shape[0])
        ka, kb = split2(keys.T)
        kt[:D, span] = ka
        kt[D:, span] = kb
        va, vb = split2(values.T)
        vt[:D, span] = va
        vt[D:, span] = vb

    def score(chunk, first, count, seen, wide):
        span = slice(first, first + count)
        k12, k13, v12 = ks.at[span, : 2 * D], ks.at[span, 2 * D :], vs.at[span, :]

        def rows_of(p):
            return pl.ds(pl.multiple_of(p * pair, pair), pair)

        def key_side(p):
            rows = rows_of(p)
            s = mm(k12[...], qt[0, :, rows]) + (mm(k12[...], qt[1, :, rows]) + mm(k13[...], qt[2, :, rows]))
            s = jnp.where(seen(count), s * scale, hidden)
            m = jnp.max(s, axis=0, keepdims=True)
            e = jnp.exp(s - m)
            sc[span, rows] = e
            top_c[chunk : chunk + 1, rows] = m
            sum_c[chunk : chunk + 1, rows] = jnp.sum(e, axis=0, keepdims=True)

        def value_side(p):
            rows = rows_of(p)
            g = mm(v12[...], ct[0, :, rows]) + mm(v12[...], ct[1, :, rows])
            dp[span, rows] = g
            dot_c[chunk : chunk + 1, rows] = jnp.sum(sc[span, rows] * g, axis=0, keepdims=True)

        def trip(i, carry):
            for k in range(wide):
                key_side(i * wide + k)
            for k in range(wide):
                value_side(i * wide + k)
            return carry

        if n_pair == wide:
            trip(0, 0)
        else:
            lax.fori_loop(0, n_pair // wide, trip, 0)

    def index_of(step):
        return lax.broadcasted_iota(jnp.int32, (step, pair), 0)

    def slot_of(step):
        return lax.broadcasted_iota(jnp.int32, (step, pair), 1) % T

    step = 256 if n_root % 256 == 0 else 128
    at_leaf = n_root + n_slice
    chunks = [(at_leaf, T)]
    chunks += [(n_root + sx * n_part, n_part) for sx in range(nx)]
    chunks += [(lo, step) for lo in range(0, n_root, step)]
    two = 2 if n_pair % 2 == 0 else 1

    stage(at_leaf, leaf_ref[0], leaf_ref[1])
    score(0, at_leaf, T, lambda step: index_of(step) <= slot_of(step), two)

    def score_part(sx):
        bb, xx = shifted(0, sx)
        first, count = chunks[1 + sx]
        stage(first, sliceb[xx, :, 0].reshape(count, D), sliceb[xx, :, 1].reshape(count, D))
        score(1 + sx, first, count, lambda step: xx * n_part + index_of(step) <= par_ref[0], two)

    if nc == 2:
        from_sibling(sliceb.at[x, other], 0)
    score_part(0)

    for sx in range(1, nx):
        bb, xx = shifted(0, nx - sx)
        blk = sliceb.at[xx, c]
        remote(blk, blk, gs_slice, gr_slice.at[sx], dev(b, x, c)).wait_recv()
        if nc == 2:
            to_sibling(blk, 1 + nx - sx)
    remote(rv_root, rv_root, gs_root, gr_root, dev(b, x, c)).wait_recv()
    if nc == 2:
        to_sibling(rootb.at[:, :, c], 1)
    for sx in range(1, nx):
        bb, xx = shifted(0, sx)
        if nc == 2:
            from_sibling(sliceb.at[xx, other], 1 + sx)
        score_part(sx)
    if nc == 2:
        from_sibling(rootb.at[:, :, other], 1)
    stage(0, rootb[:, :, :, 0].reshape(n_root, D), rootb[:, :, :, 1].reshape(n_root, D))
    for i, (first, count) in enumerate(chunks[1 + nx :]):
        score(
            1 + nx + i, first, count, lambda step: first + index_of(step) < cut_ref[0],
            n_pair if n_root == step else two,
        )

    tops = top_c[...]
    factor = jnp.exp(tops - jnp.max(tops, axis=0, keepdims=True))
    inverse = 1.0 / jnp.sum(factor * sum_c[...], axis=0, keepdims=True)
    fac_c[...] = factor * inverse
    dot_r[...] = jnp.sum(factor * dot_c[...], axis=0, keepdims=True) * inverse

    def weights(chunk, rows):
        first, count = chunks[chunk]
        span = slice(first, first + count)
        w = sc[span, rows] * fac_c[chunk : chunk + 1, rows]
        return split2(w), split2(w * ((dp[span, rows] - dot_r[:, rows]) * scale))

    def key_gradients(chunk):
        (w1, w2), (s1, s2) = weights(chunk, slice(None))
        a = mm(s1, qs[...]) + mm(s2, qs[...])
        v = mm(w1, cs[...]) + mm(w2, cs[...])
        return side(a[:, :D] + a[:, D:], v[:, :D] + v[:, D:])

    def block_gradients(chunk):
        first, count = chunks[chunk]
        dkv[first : first + count, :] = key_gradients(chunk)

    root_g = dkv.at[:n_root].reshape(nb, nx, nc, r_rows, 2 * D)
    slice_g = dkv.at[n_root : n_root + n_slice].reshape(nx, nc, b_rows, 2 * D)
    for i in range(1 + nx, len(chunks)):
        block_gradients(i)
    ex = []

    def exchange(source, target):
        if nc == 2:
            i = len(ex)
            ex.append(remote(source, target, es_sem.at[i], er_sem.at[i], dev(b, x, other)))
            ex[i].start()

    for k, sx in enumerate(columns):
        bb, xx = shifted(0, sx)
        exchange(root_g.at[:, xx, other], rc_root.at[k])
    for sx in range(nx):
        block_gradients(1 + sx)
    exchange(slice_g.at[:, other], rc_slice)
    for k, sx in enumerate(columns):
        bb, xx = shifted(0, sx)
        mine = root_g[:, xx, c]
        if nc == 2:
            ex[k].wait_recv()
            mine = mine + rc_root[k]
        sn_root[k] = mine
        for i, (sb, sy) in enumerate(peers):
            if sy == sx:
                bb, xx = shifted(sb, sx)
                remote(sn_root.at[k, bb], rv_root.at[i], ss_root, sr_root, dev(bb, xx, c)).start()

    stage_across(0, rootb[:, :, :, 0].reshape(n_root, D), rootb[:, :, :, 1].reshape(n_root, D))
    for sx in range(nx):
        bb, xx = shifted(0, sx)
        first, count = chunks[1 + sx]
        stage_across(first, sliceb[xx, :, 0].reshape(count, D), sliceb[xx, :, 1].reshape(count, D))
    stage_across(at_leaf, leaf_ref[0], leaf_ref[1])

    if nc == 2:
        ex[nx].wait_recv()
    mine = slice_g[:, c]
    sn_slice[...] = mine + rc_slice[...] if nc == 2 else mine
    for sx in range(1, nx):
        bb, xx = shifted(0, sx)
        remote(sn_slice.at[sx], rv_slice.at[sx - 1], ss_slice, sr_slice, dev(b, xx, c)).start()

    def outputs(p, carry):
        rows = pl.ds(pl.multiple_of(p * pair, pair), pair)
        m, n = None, None
        for chunk, (first, count) in enumerate(chunks):
            span = slice(first, first + count)
            (w1, w2), (s1, s2) = weights(chunk, rows)
            part = mm(vt[:, span], w1) + mm(vt[:, span], w2)
            m = part if m is None else m + part
            part = mm(kt[:, span], s1) + mm(kt[:, span], s2)
            n = part if n is None else n + part
        m = m[:D] + m[D:]
        n = n[:D] + n[D:]
        for k in range(per):
            cols = pl.ds(pl.multiple_of(p * (per * D) + k * D, D), D)
            part = slice(k * T, (k + 1) * T)
            att_ref[:, cols] = jnp.where(live, m[:, part].T, 0.0)
            dqv_ref[:, cols] = n[:, part].T
        return carry

    lax.fori_loop(0, n_pair, outputs, 0)
    dleaf_ref[...] = key_gradients(0)

    total = sn_slice[0]
    if nx > 1:
        remote(rv_slice, rv_slice, ss_slice, sr_slice, dev(b, x, c)).wait_recv()
        for i in range(nx - 1):
            total = total + rv_slice[i]
    dslice_ref[...] = total
    total = sn_root[nx - 1, b]
    if peers:
        remote(rv_root, rv_root, ss_root, sr_root, dev(b, x, c)).wait_recv()
        for i in range(len(peers)):
            total = total + rv_root[i]
    droot_ref[...] = total
    for cp in core_sends + ex:
        cp.wait_send()
    if peers:
        remote(rv_root, rv_root, gs_root, gr_root, dev(b, x, c)).wait_send()
        remote(rv_root, rv_root, ss_root, sr_root, dev(b, x, c)).wait_send()
    if nx > 1:
        remote(rv_slice, rv_slice, gs_slice, gr_slice.at[0], dev(b, x, c)).wait_send()
        remote(rv_slice, rv_slice, ss_slice, sr_slice, dev(b, x, c)).wait_send()


def deliver(*refs):
    sources, targets, sem = refs[:5], refs[5:10], refs[10]
    copies = [pltpu.make_async_copy(s, t, sem.at[i]) for i, (s, t) in enumerate(zip(sources, targets))]
    for cp in copies:
        cp.start()
    for cp in copies:
        cp.wait()


def shards(mesh, *args):
    queries, leaf_keys, _, root_keys, _, branch_keys = args[:6]
    T, width = queries.shape
    D = leaf_keys.shape[1]
    H = width // D
    r_rows, b_rows = root_keys.shape[0], branch_keys.shape[0]
    nb, nl = mesh.shape["branch"], mesh.shape["leaf"]
    nc = 2 if nl % 2 == 0 else 1
    nx = nl // nc
    R = T * H
    n_root, n_slice = nb * nl * r_rows, nl * b_rows
    n_keys = n_root + n_slice + T
    n_chunks = 1 + nx + n_root // (256 if n_root % 256 == 0 else 128)
    any_space = pl.BlockSpec(memory_space=pl.ANY)
    hbm = pl.BlockSpec(memory_space=pltpu.HBM)
    vmem = pl.BlockSpec(memory_space=pltpu.VMEM)
    V = pltpu.VMEM
    S = pltpu.SMEM
    dma = pltpu.SemaphoreType.DMA
    np_ = max(nb * nx - 1, 1)
    scratch = [
        V((2, T, width), f32), V((2, T, D), f32),
        V((nb, nx, nc, 2, r_rows, D), f32), V((nx, nc, 2, b_rows, D), f32),
        V((R, 2 * D), bf16), V((R, 2 * D), bf16), V((3, 2 * D, R), bf16), V((2, 2 * D, R), bf16),
        V((n_keys, 4 * D), bf16), V((n_keys, 2 * D), bf16),
        V((2 * D, n_keys), bf16), V((2 * D, n_keys), bf16),
        V((n_keys, R), f32), V((n_keys, R), f32), V((n_root + n_slice, 2 * D), f32),
        V((n_chunks, R), f32), V((n_chunks, R), f32), V((n_chunks, R), f32), V((n_chunks, R), f32), V((1, R), f32),
        S((1,), jnp.int32), S((1,), jnp.int32), S((1,), jnp.int32),
        V((nx, nb, r_rows, 2 * D), f32), V((nx, b_rows, 2 * D), f32),
        V((nx, nb, r_rows, 2 * D), f32), V((nx, b_rows, 2 * D), f32),
        V((np_, r_rows, 2 * D), f32), V((max(nx - 1, 1), b_rows, 2 * D), f32),
        dma((7,)), dma, dma, dma, dma((nx,)), dma((1 + nx,)), dma((1 + nx,)),
        dma, dma, dma, dma, dma((1 + nx,)), dma((1 + nx,)),
    ]
    shape = lambda *s: V(s, f32)
    sizes = ((T, width), (T, width), (r_rows, 2 * D), (b_rows, 2 * D), (T, 2 * D))
    held = pl.pallas_call(
        functools.partial(kernel, nb, nx, nc, (T, H, D, r_rows, b_rows)),
        out_shape=tuple(shape(*size) for size in sizes),
        in_specs=[any_space] * 8 + [hbm] * 3,
        out_specs=(vmem,) * 5,
        scratch_shapes=scratch,
        compiler_params=pltpu.CompilerParams(
            collective_id=0, has_side_effects=True, vmem_limit_bytes=60 * 1024 * 1024
        ),
        name="tree",
    )(*args)
    return pl.pallas_call(
        deliver,
        out_shape=tuple(jax.ShapeDtypeStruct(size, f32) for size in sizes),
        in_specs=[vmem] * 5,
        out_specs=(any_space,) * 5,
        scratch_shapes=[dma((5,))],
        compiler_params=pltpu.CompilerParams(vmem_limit_bytes=1024 * 1024),
        name="deliver",
    )(*held)


def solution(mesh):
    rows = P(("groups", "branch", "leaf"), None)
    flat = P(("groups", "branch", "leaf"))
    return jax.shard_map(
        functools.partial(shards, mesh),
        mesh=mesh,
        in_specs=(rows,) * 8 + (flat, flat, P(("groups", "branch"))),
        out_specs=(rows,) * 5,
        check_vma=False,
    )
```
